256 devices in a mesh: seq: 32 (over x, y, core), dp: 8 (over z).
Axes of the slice: x: 4, y: 4, z: 8, core: 2. Of those that a mesh axis runs over, the one named last changes fastest.
Arguments:
- queries: bfloat16 [16, 2048, 4096], P('dp', 'seq'), may hold values from -8 to 8
- unrotated_key_rows: bfloat16 [16, 2048, 1024], P('dp', 'seq'), may hold values from -8 to 8
- value_projection_rows: bfloat16 [16, 2048, 1024], P('dp', 'seq'), may hold values from -6 to 6
- attention_output_gradient: bfloat16 [16, 2048, 4096], P('dp', 'seq'), may hold values from -16 to 16
- normed_hidden_input: bfloat16 [16, 2048, 4096], P('dp', 'seq'), may hold values from -6 to 6
- adapter_down_weight: bfloat16 [4096, 64], replicated, may hold values from -0.01171875 to 0.01171875
- adapter_up_weight: bfloat16 [64, 4096], replicated, may hold values from -0.01171875 to 0.01171875
- lengths: int32 [16], P('dp'), may hold values from 1024 to 2048, as said below
- offsets: int32 [16], P('dp'), may hold values from 0 to 31
Outputs:
- grad_query: bfloat16 [16, 2048, 4096], P('dp', 'seq')
- grad_key: bfloat16 [16, 2048, 1024], P('dp', 'seq')
- grad_value: bfloat16 [16, 2048, 1024], P('dp', 'seq')
- grad_down: float32 [4096, 64], P('seq')
- grad_up: float32 [64, 4096], P(None, 'seq')
The draws below stay inside these ranges and needn't reach their ends.
Inputs may be any that keep to these rules, and one draw needn't show every extreme that they name: `lengths`: in every draw at least one rollout has all 2048 positions valid.
All inputs are finite; a program needn't handle non-finite values.
Results may differ from the reference program's by a relative error of at most 0.018.
The reference program's roundings to bfloat16 on the way count: a program that leaves them out, or rounds other values in their place, can miss the bound.
Values may be sent and summed in bfloat16 or wider, within the bound.
No kernel may reach another device: no remote copies, remote signals or barrier semaphores. Data moves between devices by JAX's collectives and lax.ppermute only.
A program may use at most 64 MiB of HBM per device.

```python
import jax
import jax.numpy as jnp
from jax import lax

MODEL_WIDTH = 4096
QUERY_HEADS = 32
KVH = 8
HEAD_WIDTH = 128
ADAPTER_RANK = 64
TOK_DEV = 64
SEQ_LEN = 2048
ROLLOUTS = 16


def draw_queries(key, part):
    drawn = jnp.clip(jax.random.normal(jax.random.fold_in(key, 1), (ROLLOUTS, SEQ_LEN, QUERY_HEADS, HEAD_WIDTH), jnp.float32), -8.0, 8.0)
    return drawn.reshape(ROLLOUTS, SEQ_LEN, QUERY_HEADS * HEAD_WIDTH).astype(jnp.bfloat16)


def draw_unrotated_key_rows(key, part):
    drawn = jnp.clip(jax.random.normal(jax.random.fold_in(key, 2), (ROLLOUTS, SEQ_LEN, KVH, HEAD_WIDTH), jnp.float32), -8.0, 8.0)
    return drawn.reshape(ROLLOUTS, SEQ_LEN, KVH * HEAD_WIDTH).astype(jnp.bfloat16)


def draw_lengths(key, part):
    picks = jax.random.randint(jax.random.fold_in(key, 21), (ROLLOUTS,), SEQ_LEN // 2, SEQ_LEN + 1)
    longest = jax.random.randint(jax.random.fold_in(key, 22), (), 0, ROLLOUTS)
    return jnp.where(jnp.arange(ROLLOUTS, dtype=jnp.int32) == longest, SEQ_LEN, picks).astype(jnp.int32)


def with_ends(values, stream_key, least, high):
    extent = values.shape
    spot = [jax.random.randint(jax.random.fold_in(stream_key, axis), (), 0, extent[axis]) for axis in range(len(extent))]
    values = values.at[tuple(spot)].set(least)
    longest = extent.index(max(extent))
    spot[longest] = (spot[longest] + 1) % extent[longest]
    return values.at[tuple(spot)].set(high)


def level_of(key, dims, cuts, least, top_value):
    level, own = 1.0, jax.random.fold_in(key, 6)
    for dim, parts in cuts:
        draws = jnp.exp(jax.random.uniform(jax.random.fold_in(own, dim), (parts,), jnp.float32, least / len(cuts), top_value / len(cuts)))
        level = level * jnp.repeat(draws, dims[dim] // parts).reshape([-1 if axis == dim else 1 for axis in range(len(dims))])
    return level


def noise(key, extent, spread, reach, pieces=(), held_as=jnp.bfloat16):
    values = jax.random.normal(key, extent, jnp.float32) * spread
    if len(pieces) > 0:
        values = level_of(key, extent, pieces, -0.22, 0.18) * values
    return jnp.clip(values, min=-reach, max=reach).astype(held_as)


def setup_inputs(seed: int = 0) -> dict:
    seeds = jax.random.split(jax.random.key(seed), 10)
    queries = draw_queries(jax.random.fold_in(seeds[9], 71), 0)
    unrotated_key_rows = draw_unrotated_key_rows(jax.random.fold_in(seeds[9], 71), 0)
    value_projection_rows = noise(seeds[2], (ROLLOUTS, SEQ_LEN, KVH * HEAD_WIDTH), 1.0, 6.0, ((0, 8), (1, 32)))
    attention_output_gradient = noise(seeds[3], (ROLLOUTS, SEQ_LEN, QUERY_HEADS * HEAD_WIDTH), 4.0, 16.0, ((0, 8), (1, 32)))
    normed_hidden_input = noise(seeds[4], (ROLLOUTS, SEQ_LEN, MODEL_WIDTH), 1.0, 6.0, ((0, 8), (1, 32)))
    adapter_down_weight = noise(seeds[5], (MODEL_WIDTH, ADAPTER_RANK), (MODEL_WIDTH * 64) ** -0.5, 0.01171875)
    adapter_up_weight = noise(seeds[6], (ADAPTER_RANK, QUERY_HEADS * HEAD_WIDTH), (QUERY_HEADS * HEAD_WIDTH * 64) ** -0.5, 0.01171875)
    lengths = draw_lengths(jax.random.fold_in(seeds[9], 71), 0)
    offsets = with_ends(jax.random.randint(seeds[8], (ROLLOUTS,), 0, TOK_DEV // 2), jax.random.fold_in(seeds[8], 1), 0, (TOK_DEV // 2) - 1).astype(jnp.int32)
    return {"queries": queries, "unrotated_key_rows": unrotated_key_rows, "value_projection_rows": value_projection_rows, "attention_output_gradient": attention_output_gradient, "normed_hidden_input": normed_hidden_input, "adapter_down_weight": adapter_down_weight, "adapter_up_weight": adapter_up_weight, "lengths": lengths, "offsets": offsets}


rotary_base = 500000.0


def rotary_tables(length, head_size):
    half_size = head_size // 2
    frequency = rotary_base ** (-(jnp.arange(half_size, dtype=jnp.float32) * 2.0 / head_size))
    angles = jnp.arange(length, dtype=jnp.float32)[:, None] * frequency[None, :]
    return jnp.cos(angles), jnp.sin(angles)


def rotate(fields, cosine, sine_table, direction):
    half_size = fields.shape[-1] // 2
    first_half = fields[..., :half_size]
    second_half = fields[..., half_size:]
    cos_wide = cosine[:, None, :]
    sin_wide = direction * sine_table[:, None, :]
    return jnp.concatenate([first_half * cos_wide - second_half * sin_wide, second_half * cos_wide + first_half * sin_wide], axis=-1)


def head_backward(rot_query, rot_key, value_head, grad_head, offset, block_rows):
    length = rot_query.shape[0]
    head_size = rot_query.shape[1]
    score_scale = head_size ** -0.5
    key_accum = jnp.zeros((length, head_size), jnp.float32)
    value_accum = jnp.zeros((length, head_size), jnp.float32)
    query_parts = []
    for block_index in range(length // block_rows):
        begin_row = block_index * block_rows
        end_row = begin_row + block_rows
        row_index = jnp.arange(begin_row, end_row, dtype=jnp.int32)[:, None]
        col_index = jnp.arange(end_row, dtype=jnp.int32)[None, :]
        visible = (col_index == row_index) | ((col_index >= offset) & (col_index <= row_index))
        query_block = rot_query[begin_row:end_row]
        grad_block = grad_head[begin_row:end_row]
        key_block = rot_key[:end_row]
        value_block = value_head[:end_row]
        scores = jnp.dot(query_block, key_block.T, preferred_element_type=jnp.float32) * score_scale
        row_max = jnp.max(jnp.where(visible, scores, -jnp.inf), axis=1, keepdims=True)
        weights_exp = jnp.where(visible, jnp.exp(scores - row_max), 0.0)
        probability = weights_exp / jnp.sum(weights_exp, axis=1, keepdims=True)
        prob_low = probability.astype(jnp.bfloat16)
        grad_prob = jnp.dot(grad_block, value_block.T, preferred_element_type=jnp.float32)
        row_delta = jnp.sum(probability * grad_prob, axis=1, keepdims=True)
        grad_score = (probability * (grad_prob - row_delta) * score_scale).astype(jnp.bfloat16)
        query_parts.append(jnp.dot(grad_score, key_block, preferred_element_type=jnp.float32))
        key_accum = key_accum.at[:end_row].add(jnp.dot(grad_score.T, query_block, preferred_element_type=jnp.float32))
        value_accum = value_accum.at[:end_row].add(jnp.dot(prob_low.T, grad_block, preferred_element_type=jnp.float32))
    return jnp.concatenate(query_parts, axis=0), key_accum, value_accum


def take_head(source, chosen_head):
    return lax.dynamic_index_in_dim(source, chosen_head, 1, keepdims=False)


def reference(queries, unrotated_key_rows, value_projection_rows, attention_output_gradient, normed_hidden_input, adapter_down_weight, adapter_up_weight, lengths, offsets):
    length = queries.shape[1]
    query_width = queries.shape[2]
    head_count = query_width // HEAD_WIDTH
    key_groups = unrotated_key_rows.shape[2] // HEAD_WIDTH
    group_size = head_count // key_groups
    block_rows = min(512, length)
    cosine, sine_table = rotary_tables(length, HEAD_WIDTH)
    positions = jnp.arange(length, dtype=jnp.int32)

    def one_rollout(inputs):
        query_sequence, key_sequence, value_sequence, grad_sequence, valid_length, offset = inputs
        keep_mask = (positions >= offset) & (positions < valid_length)
        grad_sequence = jnp.where(keep_mask[:, None], grad_sequence, jnp.zeros_like(grad_sequence))
        rot_query = rotate(query_sequence.reshape(length, head_count, HEAD_WIDTH).astype(jnp.float32), cosine, sine_table, 1.0).astype(jnp.bfloat16)
        rot_key = rotate(key_sequence.reshape(length, key_groups, HEAD_WIDTH).astype(jnp.float32), cosine, sine_table, 1.0).astype(jnp.bfloat16)
        value_heads = value_sequence.reshape(length, key_groups, HEAD_WIDTH)
        grad_heads = grad_sequence.reshape(length, head_count, HEAD_WIDTH)

        def one_head(head_index):
            key_index = head_index // group_size
            query_grad, key_grad, value_grad = head_backward(take_head(rot_query, head_index), take_head(rot_key, key_index), take_head(value_heads, key_index), take_head(grad_heads, head_index), offset, block_rows)
            query_grad = rotate(query_grad[:, None, :], cosine, sine_table, -1.0)[:, 0].astype(jnp.bfloat16)
            key_grad = rotate(key_grad[:, None, :], cosine, sine_table, -1.0)[:, 0].astype(jnp.bfloat16)
            return query_grad, key_grad, value_grad.astype(jnp.bfloat16)

        query_all, key_all, value_all = lax.map(one_head, jnp.arange(head_count, dtype=jnp.int32))
        rollout_query = jnp.transpose(query_all, (1, 0, 2)).reshape(length, query_width)
        key_sum = key_all.astype(jnp.float32).reshape(key_groups, group_size, length, HEAD_WIDTH).sum(axis=1).astype(jnp.bfloat16)
        value_sum = value_all.astype(jnp.float32).reshape(key_groups, group_size, length, HEAD_WIDTH).sum(axis=1).astype(jnp.bfloat16)
        rollout_key = jnp.transpose(key_sum, (1, 0, 2)).reshape(length, key_groups * HEAD_WIDTH)
        rollout_value = jnp.transpose(value_sum, (1, 0, 2)).reshape(length, key_groups * HEAD_WIDTH)
        return rollout_query, rollout_key, rollout_value

    grad_query, grad_key, grad_value = lax.map(one_rollout, (queries, unrotated_key_rows, value_projection_rows, attention_output_gradient, lengths, offsets))
    hidden_state = normed_hidden_input.reshape(-1, normed_hidden_input.shape[2])
    flattened_query = grad_query.reshape(-1, query_width)
    adapter_latent = jnp.dot(hidden_state, adapter_down_weight, preferred_element_type=jnp.float32).astype(jnp.bfloat16)
    backward_gradient = jnp.dot(flattened_query, adapter_up_weight.T, preferred_element_type=jnp.float32).astype(jnp.bfloat16)
    grad_down = jnp.dot(hidden_state.T, backward_gradient, preferred_element_type=jnp.float32)
    grad_up = jnp.dot(adapter_latent.T, flattened_query, preferred_element_type=jnp.float32)
    return grad_query, grad_key, grad_value, grad_down, grad_up
```

```python
import functools
import math

import jax
import jax.numpy as jnp
from jax import lax
from jax.experimental import pallas as pl
from jax.experimental.pallas import tpu as pltpu
from jax.sharding import PartitionSpec as P

HEAD = 128
BQ = 256
PAIR = 2 * HEAD
NT = (((1,), (1,)), ((), ()))
NN = (((1,), (0,)), ((), ()))
VM = pl.BlockSpec(memory_space=pltpu.VMEM)
SM = pl.BlockSpec(memory_space=pltpu.SMEM)
rotary_base = 500000.0


def rotary_tables(positions):
    half = HEAD // 2
    frequency = rotary_base ** (-(jnp.arange(half, dtype=jnp.float32) * 2.0 / HEAD))
    angles = positions.astype(jnp.float32)[:, None] * frequency[None, :]
    cos, sin = jnp.cos(angles), jnp.sin(angles)
    return jnp.concatenate([cos, cos], axis=1), jnp.concatenate([-sin, sin], axis=1)


def dot(a, b, dims):
    return lax.dot_general(a, b, dims, preferred_element_type=jnp.float32)


def turn(u, cos, sin):
    return u * cos + pltpu.roll(u, HEAD // 2, 1) * sin


def prep_kernel(place_ref, q_ref, k_ref, v_ref, g_ref, cos_ref, sin_ref, out_ref):
    tok = q_ref.shape[1]
    rollout = pl.program_id(0)
    cos, sin = cos_ref[...], sin_ref[...]
    at = place_ref[0] + lax.broadcasted_iota(jnp.int32, (tok, HEAD), 0)
    keep = (at >= place_ref[1 + rollout]) & (at < place_ref[3 + rollout])

    def turned(ref, lo):
        u = ref[0, :, lo : lo + HEAD].astype(jnp.float32)
        return turn(u, cos, sin).astype(jnp.bfloat16)

    for kv in range(k_ref.shape[2] // HEAD):
        key = turned(k_ref, kv * HEAD)
        value = v_ref[0, :, kv * HEAD : (kv + 1) * HEAD]
        for half in range(2):
            p = 2 * kv + half
            for j in range(2):
                lo = (2 * p + j) * HEAD
                out_ref[p, j * tok : (j + 1) * tok, :] = turned(q_ref, lo)
                g = g_ref[0, :, lo : lo + HEAD]
                out_ref[p, (2 + j) * tok : (3 + j) * tok, :] = jnp.where(keep, g, jnp.zeros_like(g))
            out_ref[p, 4 * tok : 5 * tok, :] = key
            out_ref[p, 5 * tok : 6 * tok, :] = value


def prepare(place, q, k, v, g, cos, sin):
    rollouts, tok, width = q.shape
    parts = 4
    pairs = width // PAIR

    def rows(a):
        return pl.BlockSpec((1, tok, a.shape[2] // parts), lambda r, i: (r, 0, i))

    table = pl.BlockSpec((tok, HEAD), lambda r, i: (0, 0))
    return pl.pallas_call(
        prep_kernel,
        grid=(rollouts, parts),
        out_shape=jax.ShapeDtypeStruct((rollouts * pairs, 6 * tok, HEAD), jnp.bfloat16),
        in_specs=[SM, rows(q), rows(k), rows(v), rows(g), table, table],
        out_specs=pl.BlockSpec((pairs // parts, 6 * tok, HEAD), lambda r, i: (r * parts + i, 0, 0)),
        name="prepare",
    )(place, q, k, v, g, cos, sin)

def attn_kernel(off_ref, x_ref, cos_ref, sin_ref, dq_ref, dkv_ref, s_ref, dp_ref, p_ref, ds_ref, dk_ref, dv_ref, k_ref, kt_ref, v_ref):
    length = dk_ref.shape[0]
    tok = x_ref.shape[1] // 6
    per = BQ // tok
    scale = HEAD ** -0.5
    c = scale * math.log2(math.e)
    off = off_ref[0]
    k_ref[...] = x_ref[:, 4 * tok : 5 * tok, :].reshape(length, HEAD)
    v_ref[...] = x_ref[:, 5 * tok : 6 * tok, :].reshape(length, HEAD)
    kt_ref[...] = k_ref[...].T
    dk_ref[...] = jnp.zeros_like(dk_ref)
    dv_ref[...] = jnp.zeros_like(dv_ref)
    for h in range(2):
        for qb in range(length // BQ):
            end = BQ * (qb + 1)
            q = x_ref[per * qb : per * (qb + 1), tok * h : tok * (h + 1), :].reshape(BQ, HEAD)
            g = x_ref[per * qb : per * (qb + 1), tok * (2 + h) : tok * (3 + h), :].reshape(BQ, HEAD)
            s_ref[:end] = dot(k_ref[:end], q, NT)
            dp_ref[:end] = dot(v_ref[:end], g, NT)
            row = lax.broadcasted_iota(jnp.int32, (BQ, BQ), 0)
            col = lax.broadcasted_iota(jnp.int32, (BQ, BQ), 1)
            last = slice(end - BQ, end)
            if qb == 0:
                seen = (row == col) | ((row >= off) & (row <= col))
                s_ref[last] = jnp.where(seen, s_ref[last], -1e30)
            else:
                s_ref[last] = jnp.where(row <= col, s_ref[last], -1e30)
                first = lax.broadcasted_iota(jnp.int32, (tok, BQ), 0)
                s_ref[:tok] = jnp.where(first >= off, s_ref[:tok], -1e30)
            top = None
            for kb in range(qb + 1):
                t = jnp.max(s_ref[BQ * kb : BQ * (kb + 1)].reshape(BQ // 8, 8, BQ), axis=0)
                top = t if top is None else jnp.maximum(top, t)
            top = jnp.max(top, axis=0, keepdims=True)
            total = jnp.zeros((8, BQ), jnp.float32)
            delta = jnp.zeros((8, BQ), jnp.float32)
            for kb in range(qb + 1):
                rows = slice(BQ * kb, BQ * (kb + 1))
                e = jnp.exp2((s_ref[rows] - top) * c)
                s_ref[rows] = e
                total += jnp.sum(e.reshape(BQ // 8, 8, BQ), axis=0)
                delta += jnp.sum((e * dp_ref[rows]).reshape(BQ // 8, 8, BQ), axis=0)
            inv = 1.0 / jnp.sum(total, axis=0, keepdims=True)
            delta = jnp.sum(delta, axis=0, keepdims=True) * inv
            for kb in range(qb + 1):
                rows = slice(BQ * kb, BQ * (kb + 1))
                p = s_ref[rows] * inv
                p_ref[rows] = p.astype(jnp.bfloat16)
                ds_ref[rows] = (p * ((dp_ref[rows] - delta) * scale)).astype(jnp.bfloat16)
            dv_ref[:end] += dot(p_ref[:end], g, NN)
            dk_ref[:end] += dot(ds_ref[:end], q, NN)
            dq = dot(kt_ref[:, :end], ds_ref[:end], NN).T
            mine = slice(BQ * qb, BQ * (qb + 1))
            dq = turn(dq, cos_ref[mine], sin_ref[mine])
            dq_ref[mine, HEAD * h : HEAD * (h + 1)] = dq.astype(jnp.bfloat16)
    dk = dk_ref[...]
    dkv_ref[:, :HEAD] = turn(dk, cos_ref[...], sin_ref[...]).astype(jnp.bfloat16)
    dkv_ref[:, HEAD:] = dv_ref[...].astype(jnp.bfloat16)


def attend(off, x, cos, sin):
    n = x.shape[0]
    length = n * x.shape[1] // 6
    vm = pl.BlockSpec(memory_space=pltpu.VMEM)
    return pl.pallas_call(
        attn_kernel,
        out_shape=(jax.ShapeDtypeStruct((length, 2 * HEAD), jnp.bfloat16),) * 2,
        in_specs=[pl.BlockSpec(memory_space=pltpu.SMEM), vm, vm, vm],
        out_specs=(vm, vm),
        scratch_shapes=[
            pltpu.VMEM((length, BQ), jnp.float32),
            pltpu.VMEM((length, BQ), jnp.float32),
            pltpu.VMEM((length, BQ), jnp.bfloat16),
            pltpu.VMEM((length, BQ), jnp.bfloat16),
            pltpu.VMEM((length, HEAD), jnp.float32),
            pltpu.VMEM((length, HEAD), jnp.float32),
            pltpu.VMEM((length, HEAD), jnp.bfloat16),
            pltpu.VMEM((HEAD, length), jnp.bfloat16),
            pltpu.VMEM((length, HEAD), jnp.bfloat16),
        ],
        compiler_params=pltpu.CompilerParams(vmem_limit_bytes=40 << 20),
        name="attend",
    )(off, x, cos, sin)

def finish_kernel(y_ref, up_ref, lat_ref, hid_ref, gq_ref, terms_ref):
    rollouts, tok, width = gq_ref.shape
    rank = up_ref.shape[0]
    pairs = width // PAIR
    for r in range(rollouts):
        for p in range(pairs):
            gq_ref[r, :, p * PAIR : (p + 1) * PAIR] = y_ref[r * pairs + p]
    flat = gq_ref[...].reshape(rollouts * tok, width)
    back = dot(flat, up_ref[...], NT).astype(jnp.bfloat16)
    hidden = hid_ref[...].reshape(rollouts * tok, width)
    down = dot(back.T, hidden, NN).astype(jnp.bfloat16)
    upper = dot(lat_ref[...].T, flat, NN).astype(jnp.bfloat16)
    for d in range(width // HEAD):
        terms_ref[d, :rank, :] = down[:, d * HEAD : (d + 1) * HEAD]
        terms_ref[d, rank:, :] = upper[:, d * HEAD : (d + 1) * HEAD]


def finish(y, up, latent, hidden):
    rollouts, tok, width = hidden.shape
    rank = up.shape[0]
    return pl.pallas_call(
        finish_kernel,
        out_shape=(
            jax.ShapeDtypeStruct((rollouts, tok, width), jnp.bfloat16),
            jax.ShapeDtypeStruct((width // HEAD, 2 * rank, HEAD), jnp.bfloat16),
        ),
        in_specs=[VM] * 4,
        out_specs=(VM, VM),
        name="finish",
    )(y, up, latent, hidden)


def keys_kernel(z_ref, gk_ref, gv_ref):
    rollouts, _, width = gk_ref.shape
    groups = width // HEAD
    for r in range(rollouts):
        for kv in range(groups):
            at = 2 * (r * groups + kv)
            both = z_ref[at].astype(jnp.float32) + z_ref[at + 1].astype(jnp.float32)
            both = both.astype(jnp.bfloat16)
            gk_ref[r, :, kv * HEAD : (kv + 1) * HEAD] = both[:, :HEAD]
            gv_ref[r, :, kv * HEAD : (kv + 1) * HEAD] = both[:, HEAD:]


def key_sums(z, shape):
    return pl.pallas_call(
        keys_kernel,
        out_shape=(jax.ShapeDtypeStruct(shape, jnp.bfloat16),) * 2,
        in_specs=[VM],
        out_specs=(VM, VM),
        name="key_sums",
    )(z)


def exchange(x, axis):
    return lax.all_to_all(x, axis, 0, 0, tiled=True)


def on_device(q, k, v, g, hidden, down, up, lengths, offsets):
    rollouts, tok, width = q.shape
    members = lax.axis_size("seq")
    length = tok * members
    me = lax.axis_index("seq")
    cos, sin = rotary_tables(me * tok + jnp.arange(tok, dtype=jnp.int32))
    place = jnp.concatenate([(me * tok)[None].astype(jnp.int32), offsets, lengths])
    x = exchange(prepare(place, q, k, v, g, cos, sin), "seq")
    flat_hidden = hidden.reshape(rollouts * tok, width)
    latent = dot(flat_hidden, down, NN).astype(jnp.bfloat16)
    cos_all, sin_all = rotary_tables(jnp.arange(length, dtype=jnp.int32))
    mine = me // (members // rollouts)
    dq, dkv = attend(lax.dynamic_slice(offsets, (mine,), (1,)), x, cos_all, -sin_all)
    y = exchange(dq.reshape(members, tok, PAIR), "seq")
    z = exchange(dkv.reshape(members, tok, PAIR), "seq")
    grad_query, terms = finish(y, up, latent, hidden)
    terms = jnp.sum(exchange(terms, "seq").astype(jnp.float32), axis=0).astype(jnp.bfloat16)
    copies = lax.axis_size("dp")
    total = exchange(jnp.broadcast_to(terms[None], (copies, *terms.shape)), "dp")
    total = jnp.sum(total.astype(jnp.float32), axis=0)
    grad_key, grad_value = key_sums(z, k.shape)
    rank = up.shape[0]
    return grad_query, grad_key, grad_value, total[:rank].T, total[rank:]


def solution(mesh):
    rows = P("dp", "seq", None)
    return jax.shard_map(
        on_device,
        mesh=mesh,
        in_specs=(rows, rows, rows, rows, rows, P(), P(), P("dp"), P("dp")),
        out_specs=(rows, rows, rows, P("seq", None), P(None, "seq")),
        check_vma=False,
    )
```

```python
import math

import jax
import jax.numpy as jnp
import numpy as np
from jax import lax
from jax.experimental import pallas as pl
from jax.experimental.pallas import tpu as pltpu
from jax.sharding import PartitionSpec as P


HEAD = 128
BQ = 256
PAIR = 2 * HEAD
NT = (((1,), (1,)), ((), ()))
NN = (((1,), (0,)), ((), ()))
VM = pl.BlockSpec(memory_space=pltpu.VMEM)
SM = pl.BlockSpec(memory_space=pltpu.SMEM)
rotary_base = 500000.0


def rotary_tables(positions):
    half = HEAD // 2
    frequency = (rotary_base ** (-(np.arange(half) * 2.0 / HEAD))).astype(np.float32)
    angles = positions.astype(jnp.float32)[:, None] * frequency[None, :]
    return jnp.concatenate([jnp.cos(angles), jnp.sin(angles)], axis=1)


def spread(table, sign):
    other = pltpu.roll(table, HEAD // 2, 1)
    low = lax.broadcasted_iota(jnp.int32, table.shape, 1) < HEAD // 2
    return jnp.where(low, table, other), jnp.where(low, -sign * other, sign * table)


def dot(a, b, dims):
    return lax.dot_general(a, b, dims, preferred_element_type=jnp.float32)


def turn(u, cos, sin):
    return u * cos + pltpu.roll(u, HEAD // 2, 1) * sin


def in_hbm(*arrays):
    return [pltpu.with_memory_space_constraint(a, pltpu.HBM) for a in arrays]


def in_vmem(*arrays):
    return [pltpu.with_memory_space_constraint(a, pltpu.VMEM) for a in arrays]


def prep_kernel(off_ref, len_ref, q_ref, k_ref, v_ref, g_ref, table_ref, out_ref):
    tok = q_ref.shape[1]
    part = tok // 2
    rollout = pl.program_id(0)
    cos, sin = spread(table_ref[...], 1.0)
    at = lax.axis_index("seq") * tok + lax.broadcasted_iota(jnp.int32, (tok, HEAD), 0)
    keep = (at >= off_ref[rollout]) & (at < len_ref[rollout])

    def turned(ref, lo):
        u = ref[0, :, lo : lo + HEAD].astype(jnp.float32)
        return turn(u, cos, sin).astype(jnp.bfloat16)

    for kv in range(k_ref.shape[2] // HEAD):
        key = turned(k_ref, kv * HEAD)
        value = v_ref[0, :, kv * HEAD : (kv + 1) * HEAD]
        for half in range(2):
            p = 2 * kv + half
            for j in range(2):
                lo = (2 * p + j) * HEAD
                out_ref[p, j * tok : (j + 1) * tok, :] = turned(q_ref, lo)
                g = g_ref[0, :, lo : lo + HEAD]
                out_ref[p, (2 + j) * tok : (3 + j) * tok, :] = jnp.where(keep, g, jnp.zeros_like(g))
            mine = slice(half * part, (half + 1) * part)
            out_ref[p, 4 * tok : 4 * tok + part, :] = key[mine]
            out_ref[p, 4 * tok + part :, :] = value[mine]


def prepare(offsets, lengths, q, k, v, g, table):
    rollouts, tok, width = q.shape
    parts = 1
    pairs = width // PAIR

    def rows(a):
        return pl.BlockSpec((1, tok, a.shape[2] // parts), lambda r, i: (r, 0, i))

    whole = pl.BlockSpec((tok, HEAD), lambda r, i: (0, 0))
    return pl.pallas_call(
        prep_kernel,
        grid=(rollouts, parts),
        out_shape=pltpu.HBM((rollouts * pairs, 5 * tok, HEAD), jnp.bfloat16),
        in_specs=[SM, SM, rows(q), rows(k), rows(v), rows(g), whole],
        out_specs=pl.BlockSpec((pairs // parts, 5 * tok, HEAD), lambda r, i: (r * parts + i, 0, 0)),
        compiler_params=pltpu.CompilerParams(vmem_limit_bytes=16 << 20),
        name="prepare",
    )(*in_hbm(offsets, lengths, q, k, v, g), table)


def attn_kernel(
    off_ref,
    x_ref,
    other_ref,
    table_hbm,
    dq_hbm,
    keep_hbm,
    give_hbm,
    table_ref,
    dq_ref,
    s_ref,
    dp_ref,
    p_ref,
    ds_ref,
    dk_ref,
    dv_ref,
    k4_ref,
    v4_ref,
    kt_ref,
    k_ref,
    v_ref,
    sum_ref,
    sems,
):
    length = dk_ref.shape[0]
    tok = x_ref.shape[1] // 5
    part = tok // 2
    place = lax.axis_index("seq")
    half = place % 2
    off = off_ref[place // (x_ref.shape[0] // off_ref.shape[0])]
    per = BQ // tok
    blocks = length // BQ
    scale = HEAD ** -0.5
    c = scale * math.log2(math.e)
    fetch = pltpu.make_async_copy(table_hbm, table_ref, sems.at[0])
    fetch.start()
    k4_ref[:, half] = x_ref[:, 4 * tok : 4 * tok + part, :]
    v4_ref[:, half] = x_ref[:, 4 * tok + part :, :]
    k4_ref[:, 1 - half] = other_ref[:, :part, :]
    v4_ref[:, 1 - half] = other_ref[:, part:, :]
    k_ref[...] = k4_ref[...].reshape(length, HEAD)
    v_ref[...] = v4_ref[...].reshape(length, HEAD)
    kt_ref[...] = k_ref[...].T
    dk_ref[...] = jnp.zeros_like(dk_ref)
    dv_ref[...] = jnp.zeros_like(dv_ref)
    units = [(h, qb) for qb in range(blocks) for h in range(2)]

    def operands(u):
        h, qb = units[u]
        at = slice(per * qb, per * (qb + 1))
        q = x_ref[at, tok * h : tok * (h + 1), :].reshape(BQ, HEAD)
        g = x_ref[at, tok * (2 + h) : tok * (3 + h), :].reshape(BQ, HEAD)
        return u % 2, BQ * (units[u][1] + 1), q, g

    def scores(u):
        b, end, q, g = operands(u)
        s_ref[b, :end] = dot(k_ref[:end], q, NT)
        dp_ref[b, :end] = dot(v_ref[:end], g, NT)

    def weigh(u):
        b, end, _, _ = operands(u)
        qb = units[u][1]
        row = lax.broadcasted_iota(jnp.int32, (BQ, BQ), 0)
        col = lax.broadcasted_iota(jnp.int32, (BQ, BQ), 1)
        last = slice(end - BQ, end)
        if qb == 0:
            seen = (row == col) | ((row >= off) & (row <= col))
            s_ref[b, last] = jnp.where(seen, s_ref[b, last], -1e30)
        else:
            s_ref[b, last] = jnp.where(row <= col, s_ref[b, last], -1e30)
            early = lax.broadcasted_iota(jnp.int32, (tok, BQ), 0)
            s_ref[b, :tok] = jnp.where(early >= off, s_ref[b, :tok], -1e30)
        top = None
        for kb in range(qb + 1):
            t = jnp.max(s_ref[b, BQ * kb : BQ * (kb + 1)].reshape(BQ // 8, 8, BQ), axis=0)
            top = t if top is None else jnp.maximum(top, t)
        top = jnp.max(top, axis=0, keepdims=True)
        total = jnp.zeros((8, BQ), jnp.float32)
        delta = jnp.zeros((8, BQ), jnp.float32)
        for kb in range(qb + 1):
            rows = slice(BQ * kb, BQ * (kb + 1))
            e = jnp.exp2((s_ref[b, rows] - top) * c)
            s_ref[b, rows] = e
            total += jnp.sum(e.reshape(BQ // 8, 8, BQ), axis=0)
            delta += jnp.sum((e * dp_ref[b, rows]).reshape(BQ // 8, 8, BQ), axis=0)
        inv = 1.0 / jnp.sum(total, axis=0, keepdims=True)
        delta = jnp.sum(delta, axis=0, keepdims=True) * inv
        for kb in range(qb + 1):
            rows = slice(BQ * kb, BQ * (kb + 1))
            e = s_ref[b, rows]
            p_ref[b, rows] = (e * inv).astype(jnp.bfloat16)
            ds_ref[b, rows] = (e * (inv * scale) * (dp_ref[b, rows] - delta)).astype(jnp.bfloat16)

    def rows_out(qb):
        mine = slice(BQ * qb, BQ * (qb + 1))
        return pltpu.make_async_copy(dq_ref.at[mine], dq_hbm.at[mine], sems.at[3 + qb])

    def spend(u):
        b, end, q, g = operands(u)
        h, qb = units[u]
        dv_ref[:end] += dot(p_ref[b, :end], g, NN)
        dk_ref[:end] += dot(ds_ref[b, :end], q, NN)
        dq = dot(kt_ref[:, :end], ds_ref[b, :end], NN).T
        mine = slice(BQ * qb, BQ * (qb + 1))
        dq = turn(dq, *spread(table_ref[mine], -1.0))
        dq_ref[mine, HEAD * h : HEAD * (h + 1)] = dq.astype(jnp.bfloat16)
        if h == 1:
            rows_out(qb).start()

    scores(0)
    fetch.wait()
    for u in range(len(units)):
        if u + 1 < len(units):
            scores(u + 1)
        weigh(u)
        spend(u)
    shape = k4_ref.shape
    sum_ref[:, :, :, :HEAD] = turn(dk_ref[...], *spread(table_ref[...], -1.0)).astype(jnp.bfloat16).reshape(shape)
    sum_ref[:, :, :, HEAD:] = dv_ref[...].astype(jnp.bfloat16).reshape(shape)
    give = pltpu.make_async_copy(sum_ref.at[:, 1 - half], give_hbm, sems.at[1])
    give.start()
    keep = pltpu.make_async_copy(sum_ref.at[:, half], keep_hbm, sems.at[2])
    keep.start()
    for qb in range(blocks):
        rows_out(qb).wait()
    give.wait()
    keep.wait()


def attend(offsets, x, other, table):
    n = x.shape[0]
    length = n * x.shape[1] // 5
    part = length // n // 2
    halves = (n, 2, part, HEAD)
    hbm = pl.BlockSpec(memory_space=pltpu.HBM)
    f32, low = jnp.float32, jnp.bfloat16
    return pl.pallas_call(
        attn_kernel,
        out_shape=(
            pltpu.HBM((length, PAIR), low),
            pltpu.HBM((n, part, PAIR), low),
            pltpu.HBM((n, part, PAIR), low),
        ),
        in_specs=[SM, VM, VM, hbm],
        out_specs=(hbm, hbm, hbm),
        scratch_shapes=[
            pltpu.VMEM((length, HEAD), f32),
            pltpu.VMEM((length, PAIR), low),
            pltpu.VMEM((2, length, BQ), f32),
            pltpu.VMEM((2, length, BQ), f32),
            pltpu.VMEM((2, length, BQ), low),
            pltpu.VMEM((2, length, BQ), low),
            pltpu.VMEM((length, HEAD), f32),
            pltpu.VMEM((length, HEAD), f32),
            pltpu.VMEM(halves, low),
            pltpu.VMEM(halves, low),
            pltpu.VMEM((HEAD, length), low),
            pltpu.VMEM((length, HEAD), low),
            pltpu.VMEM((length, HEAD), low),
            pltpu.VMEM((n, 2, part, PAIR), low),
            pltpu.SemaphoreType.DMA((3 + length // BQ,)),
        ],
        compiler_params=pltpu.CompilerParams(vmem_limit_bytes=40 << 20),
        cost_estimate=pl.CostEstimate(flops=24 * 10**9, bytes_accessed=8 << 20, transcendentals=6 * 10**6),
        name="attend",
    )(*in_hbm(offsets), *in_vmem(x, other), *in_hbm(table))


def keys_of_kernel(x_ref, out_ref):
    rows = out_ref.shape[1]
    out_ref[...] = x_ref[:, x_ref.shape[1] - rows :, :]


def keys_of(x):
    n, rows, width = x.shape
    return pl.pallas_call(
        keys_of_kernel,
        out_shape=pltpu.VMEM((n, rows // 5, width), x.dtype),
        in_specs=[VM],
        out_specs=VM,
        compiler_params=pltpu.CompilerParams(vmem_limit_bytes=8 << 20),
        name="keys_of",
    )(*in_vmem(x))


def finish_kernel(y_ref, up_ref, lat_ref, hid_ref, gq_hbm, terms_hbm, gq_ref, terms_ref, sems):
    rollouts, tok, width = gq_ref.shape
    rank = up_ref.shape[0]
    pairs = width // PAIR
    for r in range(rollouts):
        for p in range(pairs):
            gq_ref[r, :, p * PAIR : (p + 1) * PAIR] = y_ref[r * pairs + p]
    save = pltpu.make_async_copy(gq_ref, gq_hbm, sems.at[0])
    save.start()
    flat = gq_ref[...].reshape(rollouts * tok, width)
    back = dot(flat, up_ref[...], NT).astype(jnp.bfloat16).T
    latent = lat_ref[...].T
    hidden = hid_ref[...].reshape(rollouts * tok, width)
    pieces = sems.shape[0] - 1
    each = width // HEAD // pieces
    sends = []
    for i in range(pieces):
        cols = slice(i * each * HEAD, (i + 1) * each * HEAD)
        down = dot(back, hidden[:, cols], NN).astype(jnp.bfloat16)
        upper = dot(latent, flat[:, cols], NN).astype(jnp.bfloat16)
        for d in range(each):
            terms_ref[i * each + d, :rank, :] = down[:, d * HEAD : (d + 1) * HEAD]
            terms_ref[i * each + d, rank:, :] = upper[:, d * HEAD : (d + 1) * HEAD]
        at = slice(i * each, (i + 1) * each)
        sends.append(pltpu.make_async_copy(terms_ref.at[at], terms_hbm.at[at], sems.at[1 + i]))
        sends[-1].start()
    save.wait()
    for send in sends:
        send.wait()


def finish(y, up, latent, hidden):
    rollouts, tok, width = hidden.shape
    rank = up.shape[0]
    terms = (width // HEAD, 2 * rank, HEAD)
    hbm = pl.BlockSpec(memory_space=pltpu.HBM)
    return pl.pallas_call(
        finish_kernel,
        out_shape=(pltpu.HBM((rollouts, tok, width), jnp.bfloat16), pltpu.HBM(terms, jnp.bfloat16)),
        in_specs=[VM] * 4,
        out_specs=(hbm, hbm),
        scratch_shapes=[
            pltpu.VMEM((rollouts, tok, width), jnp.bfloat16),
            pltpu.VMEM(terms, jnp.bfloat16),
            pltpu.SemaphoreType.DMA((5,)),
        ],
        compiler_params=pltpu.CompilerParams(vmem_limit_bytes=16 << 20),
        name="finish",
    )(*in_vmem(y, up, latent, hidden))


def keys_kernel(z_ref, gk_ref, gv_ref):
    rollouts, tok, width = gk_ref.shape
    groups = width // HEAD
    part = tok // 2
    for r in range(rollouts):
        for kv in range(groups):
            for half in range(2):
                both = z_ref[2 * (r * groups + kv) + half]
                rows = slice(half * part, (half + 1) * part)
                gk_ref[r, rows, kv * HEAD : (kv + 1) * HEAD] = both[:, :HEAD]
                gv_ref[r, rows, kv * HEAD : (kv + 1) * HEAD] = both[:, HEAD:]


def key_sums(z, shape):
    return pl.pallas_call(
        keys_kernel,
        out_shape=(jax.ShapeDtypeStruct(shape, jnp.bfloat16),) * 2,
        in_specs=[VM],
        out_specs=(VM, VM),
        compiler_params=pltpu.CompilerParams(vmem_limit_bytes=8 << 20),
        name="key_sums",
    )(*in_vmem(z))


def exchange(x, axis):
    return lax.all_to_all(x, axis, 0, 0, tiled=True)


def swap(x, axis, bit):
    return lax.ppermute(x, axis, [(i, i ^ bit) for i in range(lax.axis_size(axis))])


def on_device(q, k, v, g, hidden, down, up, lengths, offsets):
    rollouts, tok, width = q.shape
    members = lax.axis_size("seq")
    length = tok * members
    own = rotary_tables(lax.axis_index("seq") * tok + jnp.arange(tok, dtype=jnp.int32))
    x = prepare(offsets, lengths, q, k, v, g, own)
    x = exchange(x, "seq")
    other = swap(keys_of(x), "seq", 1)
    flat_hidden = hidden.reshape(rollouts * tok, width)
    latent = dot(flat_hidden, down, NN).astype(jnp.bfloat16)
    table = rotary_tables(jnp.arange(length, dtype=jnp.int32))
    dq, keep, give = attend(offsets, x, other, table)
    y = exchange(dq.reshape(members, tok, PAIR), "seq")
    both = (keep.astype(jnp.float32) + swap(give, "seq", 1).astype(jnp.float32)).astype(jnp.bfloat16)
    grad_query, terms = finish(y, up, latent, hidden)
    terms = exchange(terms, "seq")
    both, terms = lax.optimization_barrier((both, terms))
    z = exchange(both, "seq")
    total = jnp.sum(terms.astype(jnp.float32), axis=0)
    bit = 1
    while bit < lax.axis_size("dp"):
        low = total.astype(jnp.bfloat16)
        got = swap(low, "dp", bit)
        total = low.astype(jnp.float32) + got.astype(jnp.float32)
        bit *= 2
    grad_key, grad_value = key_sums(z, k.shape)
    rank = up.shape[0]
    return grad_query, grad_key, grad_value, total[:rank].T, total[rank:]


def solution(mesh):
    rows = P("dp", "seq", None)

    return jax.shard_map(
        on_device,
        mesh=mesh,
        in_specs=(rows, rows, rows, rows, rows, P(), P(), P("dp"), P("dp")),
        out_specs=(rows, rows, rows, P("seq", None), P(None, "seq")),
        check_vma=False,
    )
```

```python
import math

import jax
import jax.numpy as jnp
import numpy as np
from jax import lax
from jax.experimental import pallas as pl
from jax.experimental.pallas import tpu as pltpu
from jax.sharding import PartitionSpec as P


HEAD = 128
BQ = 256
PAIR = 2 * HEAD
NT = (((1,), (1,)), ((), ()))
NN = (((1,), (0,)), ((), ()))
VM = pl.BlockSpec(memory_space=pltpu.VMEM)
SM = pl.BlockSpec(memory_space=pltpu.SMEM)
rotary_base = 500000.0


def rotary_tables(positions):
    half = HEAD // 2
    frequency = (rotary_base ** (-(np.arange(half) * 2.0 / HEAD))).astype(np.float32)
    angles = positions.astype(jnp.float32)[:, None] * frequency[None, :]
    return jnp.concatenate([jnp.cos(angles), jnp.sin(angles)], axis=1)


def spread(table, sign):
    other = pltpu.roll(table, HEAD // 2, 1)
    low = lax.broadcasted_iota(jnp.int32, table.shape, 1) < HEAD // 2
    return jnp.where(low, table, other), jnp.where(low, -sign * other, sign * table)


def dot(a, b, dims):
    return lax.dot_general(a, b, dims, preferred_element_type=jnp.float32)


def turn(u, cos, sin):
    return u * cos + pltpu.roll(u, HEAD // 2, 1) * sin


def in_hbm(*arrays):
    return [pltpu.with_memory_space_constraint(a, pltpu.HBM) for a in arrays]


def in_vmem(*arrays):
    return [pltpu.with_memory_space_constraint(a, pltpu.VMEM) for a in arrays]


def prep_kernel(off_ref, len_ref, q_ref, k_ref, v_ref, g_ref, table_ref, out_ref):
    tok = q_ref.shape[1]
    part = tok // 2
    rollout = pl.program_id(0)
    cos, sin = spread(table_ref[...], 1.0)
    at = lax.axis_index("seq") * tok + lax.broadcasted_iota(jnp.int32, (tok, HEAD), 0)
    keep = (at >= off_ref[rollout]) & (at < len_ref[rollout])

    def turned(ref, lo):
        u = ref[0, :, lo : lo + HEAD].astype(jnp.float32)
        return turn(u, cos, sin).astype(jnp.bfloat16)

    for kv in range(k_ref.shape[2] // HEAD):
        key = turned(k_ref, kv * HEAD)
        value = v_ref[0, :, kv * HEAD : (kv + 1) * HEAD]
        for half in range(2):
            p = 2 * kv + half
            for j in range(2):
                lo = (2 * p + j) * HEAD
                out_ref[p, j * tok : (j + 1) * tok, :] = turned(q_ref, lo)
                g = g_ref[0, :, lo : lo + HEAD]
                out_ref[p, (2 + j) * tok : (3 + j) * tok, :] = jnp.where(keep, g, jnp.zeros_like(g))
            mine = slice(half * part, (half + 1) * part)
            out_ref[p, 4 * tok : 4 * tok + part, :] = key[mine]
            out_ref[p, 4 * tok + part :, :] = value[mine]


def prepare(offsets, lengths, q, k, v, g, table):
    rollouts, tok, width = q.shape
    parts = 1
    pairs = width // PAIR

    def rows(a):
        return pl.BlockSpec((1, tok, a.shape[2] // parts), lambda r, i: (r, 0, i))

    whole = pl.BlockSpec((tok, HEAD), lambda r, i: (0, 0))
    return pl.pallas_call(
        prep_kernel,
        grid=(rollouts, parts),
        out_shape=pltpu.HBM((rollouts * pairs, 5 * tok, HEAD), jnp.bfloat16),
        in_specs=[SM, SM, rows(q), rows(k), rows(v), rows(g), whole],
        out_specs=pl.BlockSpec((pairs // parts, 5 * tok, HEAD), lambda r, i: (r * parts + i, 0, 0)),
        compiler_params=pltpu.CompilerParams(vmem_limit_bytes=16 << 20),
        name="prepare",
    )(*in_hbm(offsets, lengths, q, k, v, g), table)


def attn_kernel(
    off_ref,
    x_ref,
    other_ref,
    table_hbm,
    dq_hbm,
    keep_hbm,
    give_hbm,
    table_ref,
    dq_ref,
    s_ref,
    dp_ref,
    p_ref,
    ds_ref,
    dk_ref,
    dv_ref,
    k4_ref,
    v4_ref,
    kt_ref,
    k_ref,
    v_ref,
    sum_ref,
    sems,
):
    length = dk_ref.shape[0]
    tok = x_ref.shape[1] // 5
    part = tok // 2
    place = lax.axis_index("seq")
    half = place % 2
    off = off_ref[place // (x_ref.shape[0] // off_ref.shape[0])]
    per = BQ // tok
    blocks = length // BQ
    scale = HEAD ** -0.5
    c = scale * math.log2(math.e)
    fetch = pltpu.make_async_copy(table_hbm, table_ref, sems.at[0])
    fetch.start()
    for rows_ref, lo in ((k4_ref, 0), (v4_ref, part)):
        mine = x_ref[:, 4 * tok + lo : 4 * tok + lo + part, :]
        theirs = other_ref[:, lo : lo + part, :]
        rows_ref[:, 0] = jnp.where(half == 0, mine, theirs)
        rows_ref[:, 1] = jnp.where(half == 0, theirs, mine)
    k_ref[...] = k4_ref[...].reshape(length, HEAD)
    v_ref[...] = v4_ref[...].reshape(length, HEAD)
    kt_ref[...] = k_ref[...].T
    dk_ref[...] = jnp.zeros_like(dk_ref)
    dv_ref[...] = jnp.zeros_like(dv_ref)
    wide = 2 * BQ

    def operands(qb):
        at = slice(per * qb, per * (qb + 1))
        rows = [x_ref[at, tok * i : tok * (i + 1), :].reshape(BQ, HEAD) for i in range(4)]
        q = jnp.concatenate(rows[:2], axis=0)
        return qb % 2, BQ * (qb + 1), q, jnp.concatenate(rows[2:], axis=0)

    def scores(qb):
        b, end, q, g = operands(qb)
        s_ref[b, :end] = dot(k_ref[:end], q, NT)
        dp_ref[b, :end] = dot(v_ref[:end], g, NT)

    def weigh(qb):
        b, end = qb % 2, BQ * (qb + 1)
        row = lax.broadcasted_iota(jnp.int32, (BQ, wide), 0)
        col = lax.broadcasted_iota(jnp.int32, (BQ, wide), 1) % BQ
        last = slice(end - BQ, end)
        if qb == 0:
            seen = (row == col) | ((row >= off) & (row <= col))
            s_ref[b, last] = jnp.where(seen, s_ref[b, last], -1e30)
        else:
            s_ref[b, last] = jnp.where(row <= col, s_ref[b, last], -1e30)
            early = lax.broadcasted_iota(jnp.int32, (tok, wide), 0)
            s_ref[b, :tok] = jnp.where(early >= off, s_ref[b, :tok], -1e30)
        top = None
        for kb in range(qb + 1):
            t = jnp.max(s_ref[b, BQ * kb : BQ * (kb + 1)].reshape(BQ // 8, 8, wide), axis=0)
            top = t if top is None else jnp.maximum(top, t)
        top = jnp.max(top, axis=0, keepdims=True)
        total = jnp.zeros((8, wide), jnp.float32)
        delta = jnp.zeros((8, wide), jnp.float32)
        for kb in range(qb + 1):
            rows = slice(BQ * kb, BQ * (kb + 1))
            e = jnp.exp2((s_ref[b, rows] - top) * c)
            s_ref[b, rows] = e
            total += jnp.sum(e.reshape(BQ // 8, 8, wide), axis=0)
            delta += jnp.sum((e * dp_ref[b, rows]).reshape(BQ // 8, 8, wide), axis=0)
        inv = 1.0 / jnp.sum(total, axis=0, keepdims=True)
        delta = jnp.sum(delta, axis=0, keepdims=True) * inv
        for kb in range(qb + 1):
            rows = slice(BQ * kb, BQ * (kb + 1))
            e = s_ref[b, rows]
            p_ref[b, rows] = (e * inv).astype(jnp.bfloat16)
            ds_ref[b, rows] = (e * (inv * scale) * (dp_ref[b, rows] - delta)).astype(jnp.bfloat16)

    def rows_out(qb):
        mine = slice(BQ * qb, BQ * (qb + 1))
        return pltpu.make_async_copy(dq_ref.at[mine], dq_hbm.at[mine], sems.at[3 + qb])

    def spend(qb):
        b, end, q, g = operands(qb)
        dv_ref[:end] += dot(p_ref[b, :end], g, NN)
        dk_ref[:end] += dot(ds_ref[b, :end], q, NN)
        dq = dot(kt_ref[:, :end], ds_ref[b, :end], NN).T
        mine = slice(BQ * qb, BQ * (qb + 1))
        tables = spread(table_ref[mine], -1.0)
        for h in range(2):
            turned = turn(dq[h * BQ : (h + 1) * BQ], *tables)
            dq_ref[mine, HEAD * h : HEAD * (h + 1)] = turned.astype(jnp.bfloat16)
        rows_out(qb).start()

    scores(0)
    fetch.wait()
    for qb in range(blocks):
        if qb + 1 < blocks:
            scores(qb + 1)
        weigh(qb)
        spend(qb)
    shape = k4_ref.shape
    sum_ref[:, :, :, :HEAD] = turn(dk_ref[...], *spread(table_ref[...], -1.0)).astype(jnp.bfloat16).reshape(shape)
    sum_ref[:, :, :, HEAD:] = dv_ref[...].astype(jnp.bfloat16).reshape(shape)
    give = pltpu.make_async_copy(sum_ref.at[:, 1 - half], give_hbm, sems.at[1])
    give.start()
    keep = pltpu.make_async_copy(sum_ref.at[:, half], keep_hbm, sems.at[2])
    keep.start()
    for qb in range(blocks):
        rows_out(qb).wait()
    give.wait()
    keep.wait()


def attend(offsets, x, other, table):
    n = x.shape[0]
    length = n * x.shape[1] // 5
    part = length // n // 2
    halves = (n, 2, part, HEAD)
    hbm = pl.BlockSpec(memory_space=pltpu.HBM)
    f32, low = jnp.float32, jnp.bfloat16
    return pl.pallas_call(
        attn_kernel,
        out_shape=(
            pltpu.HBM((length, PAIR), low),
            pltpu.HBM((n, part, PAIR), low),
            pltpu.HBM((n, part, PAIR), low),
        ),
        in_specs=[SM, VM, VM, hbm],
        out_specs=(hbm, hbm, hbm),
        scratch_shapes=[
            pltpu.VMEM((length, HEAD), f32),
            pltpu.VMEM((length, PAIR), low),
            pltpu.VMEM((2, length, 2 * BQ), f32),
            pltpu.VMEM((2, length, 2 * BQ), f32),
            pltpu.VMEM((2, length, 2 * BQ), low),
            pltpu.VMEM((2, length, 2 * BQ), low),
            pltpu.VMEM((length, HEAD), f32),
            pltpu.VMEM((length, HEAD), f32),
            pltpu.VMEM(halves, low),
            pltpu.VMEM(halves, low),
            pltpu.VMEM((HEAD, length), low),
            pltpu.VMEM((length, HEAD), low),
            pltpu.VMEM((length, HEAD), low),
            pltpu.VMEM((n, 2, part, PAIR), low),
            pltpu.SemaphoreType.DMA((3 + length // BQ,)),
        ],
        compiler_params=pltpu.CompilerParams(vmem_limit_bytes=44 << 20),
        cost_estimate=pl.CostEstimate(flops=24 * 10**9, bytes_accessed=8 << 20, transcendentals=6 * 10**6),
        name="attend",
    )(*in_hbm(offsets), *in_vmem(x, other), *in_hbm(table))


def keys_of_kernel(x_ref, out_ref):
    rows = out_ref.shape[1]
    out_ref[...] = x_ref[:, x_ref.shape[1] - rows :, :]


def keys_of(x):
    n, rows, width = x.shape
    return pl.pallas_call(
        keys_of_kernel,
        out_shape=pltpu.VMEM((n, rows // 5, width), x.dtype),
        in_specs=[VM],
        out_specs=VM,
        compiler_params=pltpu.CompilerParams(vmem_limit_bytes=8 << 20),
        name="keys_of",
    )(*in_vmem(x))


def finish_kernel(y_ref, up_ref, lat_ref, hid_ref, gq_hbm, terms_hbm, gq_ref, terms_ref, sems):
    rollouts, tok, width = gq_ref.shape
    rank = up_ref.shape[0]
    pairs = width // PAIR
    for r in range(rollouts):
        for p in range(pairs):
            gq_ref[r, :, p * PAIR : (p + 1) * PAIR] = y_ref[r * pairs + p]
    save = pltpu.make_async_copy(gq_ref, gq_hbm, sems.at[0])
    save.start()
    flat = gq_ref[...].reshape(rollouts * tok, width)
    back = dot(flat, up_ref[...], NT).astype(jnp.bfloat16).T
    latent = lat_ref[...].T
    hidden = hid_ref[...].reshape(rollouts * tok, width)
    pieces = sems.shape[0] - 1
    each = width // HEAD // pieces
    sends = []
    for i in range(pieces):
        cols = slice(i * each * HEAD, (i + 1) * each * HEAD)
        down = dot(back, hidden[:, cols], NN).astype(jnp.bfloat16)
        upper = dot(latent, flat[:, cols], NN).astype(jnp.bfloat16)
        for d in range(each):
            terms_ref[i * each + d, :rank, :] = down[:, d * HEAD : (d + 1) * HEAD]
            terms_ref[i * each + d, rank:, :] = upper[:, d * HEAD : (d + 1) * HEAD]
        at = slice(i * each, (i + 1) * each)
        sends.append(pltpu.make_async_copy(terms_ref.at[at], terms_hbm.at[at], sems.at[1 + i]))
        sends[-1].start()
    save.wait()
    for send in sends:
        send.wait()


def finish(y, up, latent, hidden):
    rollouts, tok, width = hidden.shape
    rank = up.shape[0]
    terms = (width // HEAD, 2 * rank, HEAD)
    hbm = pl.BlockSpec(memory_space=pltpu.HBM)
    return pl.pallas_call(
        finish_kernel,
        out_shape=(pltpu.HBM((rollouts, tok, width), jnp.bfloat16), pltpu.HBM(terms, jnp.bfloat16)),
        in_specs=[VM] * 4,
        out_specs=(hbm, hbm),
        scratch_shapes=[
            pltpu.VMEM((rollouts, tok, width), jnp.bfloat16),
            pltpu.VMEM(terms, jnp.bfloat16),
            pltpu.SemaphoreType.DMA((5,)),
        ],
        compiler_params=pltpu.CompilerParams(vmem_limit_bytes=16 << 20),
        name="finish",
    )(*in_vmem(y, up, latent, hidden))


def keys_kernel(z_ref, gk_ref, gv_ref):
    rollouts, tok, width = gk_ref.shape
    groups = width // HEAD
    part = tok // 2
    for r in range(rollouts):
        for kv in range(groups):
            for half in range(2):
                both = z_ref[2 * (r * groups + kv) + half]
                rows = slice(half * part, (half + 1) * part)
                gk_ref[r, rows, kv * HEAD : (kv + 1) * HEAD] = both[:, :HEAD]
                gv_ref[r, rows, kv * HEAD : (kv + 1) * HEAD] = both[:, HEAD:]


def key_sums(z, shape):
    return pl.pallas_call(
        keys_kernel,
        out_shape=(jax.ShapeDtypeStruct(shape, jnp.bfloat16),) * 2,
        in_specs=[VM],
        out_specs=(VM, VM),
        compiler_params=pltpu.CompilerParams(vmem_limit_bytes=8 << 20),
        name="key_sums",
    )(*in_vmem(z))


def exchange(x, axis):
    return lax.all_to_all(x, axis, 0, 0, tiled=True)


def swap(x, axis, bit):
    return lax.ppermute(x, axis, [(i, i ^ bit) for i in range(lax.axis_size(axis))])


def on_device(q, k, v, g, hidden, down, up, lengths, offsets):
    rollouts, tok, width = q.shape
    members = lax.axis_size("seq")
    length = tok * members
    own = rotary_tables(lax.axis_index("seq") * tok + jnp.arange(tok, dtype=jnp.int32))
    x = prepare(offsets, lengths, q, k, v, g, own)
    x = exchange(x, "seq")
    other = swap(keys_of(x), "seq", 1)
    flat_hidden = hidden.reshape(rollouts * tok, width)
    latent = dot(flat_hidden, down, NN).astype(jnp.bfloat16)
    table = rotary_tables(jnp.arange(length, dtype=jnp.int32))
    dq, keep, give = attend(offsets, x, other, table)
    y = exchange(dq.reshape(members, tok, PAIR), "seq")
    both = (keep.astype(jnp.float32) + swap(give, "seq", 1).astype(jnp.float32)).astype(jnp.bfloat16)
    grad_query, terms = finish(y, up, latent, hidden)
    terms = exchange(terms, "seq")
    both, terms = lax.optimization_barrier((both, terms))
    z = exchange(both, "seq")
    total = jnp.sum(terms.astype(jnp.float32), axis=0)
    bit = 1
    while bit < lax.axis_size("dp"):
        low = total.astype(jnp.bfloat16)
        got = swap(low, "dp", bit)
        total = low.astype(jnp.float32) + got.astype(jnp.float32)
        bit *= 2
    grad_key, grad_value = key_sums(z, k.shape)
    rank = up.shape[0]
    return grad_query, grad_key, grad_value, total[:rank].T, total[rank:]


def solution(mesh):
    rows = P("dp", "seq", None)

    return jax.shard_map(
        on_device,
        mesh=mesh,
        in_specs=(rows, rows, rows, rows, rows, P(), P(), P("dp"), P("dp")),
        out_specs=(rows, rows, rows, P("seq", None), P(None, "seq")),
        check_vma=False,
    )
```
